32 devices in a mesh: expert: 4 (over x, core), shard: 8 (over z, y).
Axes of the slice: x: 2, y: 2, z: 4, core: 2. Of those that a mesh axis runs over, the one named last changes fastest.
Arguments:
- tokens: bfloat16 [256, 4096], P(('expert', 'shard')), may hold values from -6 to 6
- router: bfloat16 [4096, 4], replicated, may hold values from -0.09375 to 0.09375
- expert_ids: int32 [256, 2], P(('expert', 'shard')), may hold values from 0 to 3, as said below
- w_gate: bfloat16 [4, 4096, 14336], P('expert', None, 'shard'), may hold values from -0.09375 to 0.09375
- w_up: bfloat16 [4, 4096, 14336], P('expert', None, 'shard'), may hold values from -0.09375 to 0.09375
- w_down: bfloat16 [4, 14336, 4096], P('expert', 'shard'), may hold values from -0.046875 to 0.046875
Outputs:
- mixed: bfloat16 [256, 4096], P(('expert', 'shard'))
The draws below stay inside these ranges and needn't reach their ends.
Inputs may be any that keep to these rules, and one draw needn't show every extreme that they name: `expert_ids`: each row names 2 different experts. Within the rows of one device no expert is named more than 4 times, and on every device some expert is named exactly 4 times.
All inputs are finite; a program needn't handle non-finite values.
Results may differ from the reference program's by a relative error of at most 0.0074.
Values may be sent and summed in bfloat16 or wider, within the bound.
No kernel may reach another device: no remote copies, remote signals or barrier semaphores. Data moves between devices by JAX's collectives and lax.ppermute only.
A program may use at most 128 MiB of HBM per device.

```python
import jax
import jax.numpy as jnp
from jax import lax

D = 4096
FF = 14336
TOP = 2
TOK_DEV = 8
EXPERTS = 4
CAP = 4
TOKENS = 256


def draw_expert_ids(key, part):
    blocks = TOKENS // TOK_DEV
    base_key = jax.random.fold_in(key, 11)
    key_offset, key_order, key_swap = jax.random.split(base_key, 3)
    block_index = jnp.arange(blocks, dtype=jnp.int32)
    random_offset = jax.random.randint(key_offset, (blocks,), 0, EXPERTS, dtype=jnp.int32)
    offset = jnp.where(block_index % 2 == 1, random_offset, block_index % EXPERTS)
    token_index = jnp.arange(TOK_DEV, dtype=jnp.int32)
    upper = (token_index >= CAP).astype(jnp.int32)
    order_keys = jax.random.split(key_order, blocks)
    orders = jax.vmap(lambda k: jax.random.permutation(k, TOK_DEV))(order_keys).astype(jnp.int32)
    placed = upper[orders]
    first = (offset[:, None] + placed) % EXPERTS
    second = (offset[:, None] + 2 + placed) % EXPERTS
    swapped = jax.random.randint(key_swap, (blocks, TOK_DEV), 0, 2, dtype=jnp.int32)
    lead = jnp.where(swapped == 1, second, first)
    trail = jnp.where(swapped == 1, first, second)
    return jnp.stack([lead, trail], axis=2).reshape(TOKENS, TOP).astype(jnp.int32)


def block_levels(key, extent, shards, smallest, largest):
    factor_of, own = 1.0, jax.random.fold_in(key, 6)
    for dim, blocks in shards:
        heights = jnp.exp(jax.random.uniform(jax.random.fold_in(own, dim), (blocks,), jnp.float32, smallest / len(shards), largest / len(shards)))
        factor_of = factor_of * jnp.repeat(heights, extent[dim] // blocks).reshape([-1 if axis == dim else 1 for axis in range(len(extent))])
    return factor_of


def scatter_about(stream_key, shape, spread, reach, pieces=(), kind=jnp.bfloat16):
    loudness = block_levels(stream_key, shape, pieces, -0.22, 0.18) if pieces else 1.0
    drawn = jax.random.normal(stream_key, shape, jnp.float32) * spread * loudness
    return jnp.minimum(jnp.maximum(drawn, -reach), reach).astype(kind)


def setup_inputs(seed: int = 0) -> dict:
    key_list = jax.random.split(jax.random.key(seed), 7)
    tokens = scatter_about(key_list[0], (TOKENS, D), 1.0, 6.0, ((0, 32),))
    router = scatter_about(key_list[1], (D, EXPERTS), D ** -0.5, 0.09375)
    expert_ids = draw_expert_ids(jax.random.fold_in(key_list[6], 71), 0)
    w_gate = scatter_about(key_list[3], (EXPERTS, D, FF), D ** -0.5, 0.09375, ((0, 4), (2, 8)))
    w_up = scatter_about(key_list[4], (EXPERTS, D, FF), D ** -0.5, 0.09375, ((0, 4), (2, 8)))
    w_down = scatter_about(key_list[5], (EXPERTS, FF, D), FF ** -0.5, 0.046875, ((0, 4), (1, 8)))
    return {"tokens": tokens, "router": router, "expert_ids": expert_ids, "w_gate": w_gate, "w_up": w_up, "w_down": w_down}


def expert_layer(packed):
    rows, gate_w, up_w, down_w = packed
    gate = jnp.dot(rows, gate_w, preferred_element_type=jnp.float32)
    up = jnp.dot(rows, up_w, preferred_element_type=jnp.float32)
    hidden = (jax.nn.silu(gate) * up).astype(jnp.bfloat16)
    return jnp.dot(hidden, down_w, preferred_element_type=jnp.float32).astype(jnp.bfloat16)


def reference(tokens, router, expert_ids, w_gate, w_up, w_down):
    blocks = TOKENS // TOK_DEV
    logits = jnp.dot(tokens, router, preferred_element_type=jnp.float32)
    chosen = jnp.take_along_axis(logits, expert_ids, axis=1)
    first = 1.0 / (1.0 + jnp.exp(-(chosen[:, 0] - chosen[:, 1])))
    gates = jnp.stack([first, 1.0 - first], axis=1)
    grouped = expert_ids.reshape(blocks, TOK_DEV * TOP)
    onehot = (grouped[:, :, None] == jnp.arange(EXPERTS, dtype=jnp.int32)[None, None, :]).astype(jnp.int32)
    before = jnp.cumsum(onehot, axis=1) - onehot
    slots = jnp.sum(before * onehot, axis=2)
    block_ids = jnp.broadcast_to(jnp.arange(blocks, dtype=jnp.int32)[:, None], (blocks, TOK_DEV * TOP))
    positions = (block_ids * CAP + slots).reshape(-1).astype(jnp.int32)
    owners = grouped.reshape(-1).astype(jnp.int32)
    token_index = jnp.repeat(jnp.arange(TOKENS, dtype=jnp.int32), TOP)
    buffer = jnp.zeros((EXPERTS, blocks * CAP, D), jnp.bfloat16)
    buffer = buffer.at[owners, positions].set(tokens[token_index])
    results = lax.map(expert_layer, (buffer, w_gate, w_up, w_down))
    picked = results[owners, positions].reshape(TOKENS, TOP, D).astype(jnp.float32)
    mixed = jnp.sum(gates[:, :, None] * picked, axis=1)
    return mixed.astype(jnp.bfloat16)
```

```python
import functools

import jax
import jax.numpy as jnp
from jax import lax
from jax.experimental import pallas as pl
from jax.experimental.pallas import tpu as pltpu
from jax.sharding import PartitionSpec as P


LANES = 128
HIDDEN_TILE = 256
OUT_TILE = 256
MIB = 1 << 20


def cost(flops, moved):
    return pl.CostEstimate(flops=int(flops), bytes_accessed=int(moved), transcendentals=0)


def dot(a, b, contract=(1, 0)):
    dims = (((contract[0],), (contract[1],)), ((), ()))
    return lax.dot_general(a, b, dims, preferred_element_type=jnp.float32)


def line_split(count):
    inner = 1
    while inner * inner * 4 <= count:
        inner *= 2
    return count // inner, inner


def swap(value, experts, shards, expert_bits, shard_bits):
    pairs = [
        (e * shards + s, (e ^ expert_bits) * shards + (s ^ shard_bits))
        for e in range(experts)
        for s in range(shards)
    ]
    return lax.ppermute(value, ("expert", "shard"), pairs)


def picks(ids_by_lane, first_expert, n_experts, blocks, slots_per):
    per_block = 2 * slots_per
    n_tokens = blocks * per_block
    rows = n_experts * blocks * slots_per
    row = lax.broadcasted_iota(jnp.int32, (rows, n_tokens), 0)
    token = lax.broadcasted_iota(jnp.int32, (rows, n_tokens), 1)
    expert = (first_expert ^ (row // (blocks * slots_per))).astype(jnp.float32)
    block = (row // slots_per) % blocks
    slot = (row % slots_per).astype(jnp.float32)
    is_first = ids_by_lane[0:1, :] == expert
    names = jnp.where(is_first | (ids_by_lane[1:2, :] == expert), 1.0, 0.0)
    earlier_token = lax.broadcasted_iota(jnp.int32, (n_tokens, n_tokens), 0)
    later_token = lax.broadcasted_iota(jnp.int32, (n_tokens, n_tokens), 1)
    earlier = jnp.where(
        (earlier_token < later_token)
        & (earlier_token // per_block == later_token // per_block),
        1.0,
        0.0,
    )
    before = dot(names.astype(jnp.bfloat16), earlier.astype(jnp.bfloat16))
    chosen = jnp.where((token // per_block == block) & (before == slot), names, 0.0)
    return chosen, is_first


def ids_to_lanes(packed_ids):
    n_tokens = packed_ids.shape[0]
    eye = lax.broadcasted_iota(jnp.int32, (n_tokens, n_tokens), 0) == lax.broadcasted_iota(
        jnp.int32, (n_tokens, n_tokens), 1
    )
    return dot(packed_ids, jnp.where(eye, 1.0, 0.0).astype(jnp.bfloat16), (0, 0))


def gather_blocks(refs):
    return jnp.concatenate([ref[...].astype(jnp.float32) for ref in refs], axis=0).astype(
        jnp.bfloat16
    )


def dispatch_kernel(blocks, n_experts, width, *refs):
    packed = gather_blocks(refs[:blocks])
    out_refs = refs[blocks:]
    slots_per = packed.shape[0] // blocks // 2
    per_expert = blocks * slots_per
    lanes = ids_to_lanes(packed[:, width:])
    chosen, _ = picks(lanes, lax.axis_index("expert"), n_experts, blocks, slots_per)
    rows = dot(chosen.astype(jnp.bfloat16), packed[:, :width]).astype(jnp.bfloat16)
    for k in range(n_experts):
        out_refs[k][...] = rows[k * per_expert : (k + 1) * per_expert]


def gates_kernel(blocks, n_experts, width, *refs):
    router_ref, weight_ref = refs[blocks : blocks + 2]
    high_ref, low_ref, held_ref, sem = refs[blocks + 2 :]
    copy = pltpu.make_async_copy(weight_ref, held_ref, sem)
    copy.start()
    packed = gather_blocks(refs[:blocks])
    slots_per = packed.shape[0] // blocks // 2
    lanes = ids_to_lanes(packed[:, width:])
    chosen, is_first = picks(lanes, lax.axis_index("expert"), n_experts, blocks, slots_per)
    logits = dot(router_ref[...], packed[:, :width], (1, 1))
    expert = lax.broadcasted_iota(jnp.int32, logits.shape, 0).astype(jnp.float32)
    first = jnp.sum(jnp.where(lanes[0:1, :] == expert, logits, 0.0), axis=0, keepdims=True)
    second = jnp.sum(jnp.where(lanes[1:2, :] == expert, logits, 0.0), axis=0, keepdims=True)
    gate = 1.0 / (1.0 + jnp.exp(-(first - second)))
    weights = chosen * jnp.where(is_first, gate, 1.0 - gate)
    high = weights.astype(jnp.bfloat16)
    high_ref[...] = high
    low_ref[...] = (weights - high.astype(jnp.float32)).astype(jnp.bfloat16)
    copy.wait()


def hold_kernel(weight_ref, held_ref, sem):
    copy = pltpu.make_async_copy(weight_ref, held_ref, sem)
    copy.start()
    copy.wait()


def ffn_kernel(parts, *refs):
    row_refs = refs[:parts]
    gate_ref, up_ref, down_ref = refs[parts : parts + 3]
    out_refs = refs[parts + 3 : 2 * parts + 3]
    down_held, rows, hidden, sems = refs[2 * parts + 3 :]
    out_tile = down_held.shape[2]
    tiles = down_held.shape[0]

    def down_copy(tile):
        columns = pl.ds(pl.multiple_of(tile * out_tile, out_tile), out_tile)
        return pltpu.make_async_copy(down_ref.at[:, columns], down_held.at[tile], sems.at[tile])

    for tile in range(tiles):
        down_copy(tile).start()
    per_part = row_refs[0].shape[0]
    for part in range(parts):
        rows[pl.ds(part * per_part, per_part), :] = row_refs[part][...]

    n_hidden = hidden.shape[1]
    hidden_tile = HIDDEN_TILE if n_hidden % HIDDEN_TILE == 0 else LANES

    @pl.loop(0, n_hidden // hidden_tile)
    def _(tile):
        columns = pl.ds(pl.multiple_of(tile * hidden_tile, hidden_tile), hidden_tile)
        gate = dot(rows[...], gate_ref[:, columns])
        up = dot(rows[...], up_ref[:, columns])
        hidden[:, columns] = (gate / (1.0 + jnp.exp(-gate)) * up).astype(jnp.bfloat16)

    @pl.loop(0, tiles)
    def _(tile):
        down_copy(tile).wait()
        columns = pl.ds(pl.multiple_of(tile * out_tile, out_tile), out_tile)
        result = dot(hidden[...], down_held[tile]).astype(jnp.bfloat16)
        for part in range(parts):
            out_refs[part][:, columns] = result[part * per_part : (part + 1) * per_part]


def combine_kernel(parts, n_experts, blocks, *refs):
    part_refs = refs[:parts]
    high_ref, low_ref = refs[parts : parts + 2]
    out_refs = refs[parts + 2 :]
    inner = parts // n_experts
    rows = jnp.concatenate([ref[...] for ref in part_refs], axis=0)
    high = jnp.concatenate([high_ref[...]] * inner, axis=0)
    low = jnp.concatenate([low_ref[...]] * inner, axis=0)
    mixed = dot(high, rows, (0, 0)) + dot(low, rows, (0, 0))
    per_block = mixed.shape[0] // blocks
    for block in range(blocks):
        out_refs[block][...] = mixed[block * per_block : (block + 1) * per_block].astype(
            jnp.bfloat16
        )


def final_kernel(*refs):
    total = refs[0][...].astype(jnp.float32)
    for ref in refs[1:-1]:
        total = total + ref[...].astype(jnp.float32)
    refs[-1][...] = total.astype(jnp.bfloat16)


def shards_program(n_expert_axis, n_shard_axis, tokens, router, expert_ids, w_gate, w_up, w_down):
    local_tokens, width = tokens.shape
    n_experts = router.shape[1]
    outer, inner = line_split(n_shard_axis)
    slots_per = local_tokens // 2
    per_expert = outer * slots_per
    parts = inner * n_experts
    n_rows = parts * per_expert
    gathered = outer * local_tokens
    n_hidden = w_gate.shape[2]
    bf16 = jnp.bfloat16
    vmem = pl.BlockSpec(memory_space=pltpu.VMEM)
    hbm = pl.BlockSpec(memory_space=pltpu.HBM)
    exchange = functools.partial(swap, experts=n_expert_axis, shards=n_shard_axis)

    ids = jnp.pad(expert_ids.astype(bf16), ((0, 0), (0, LANES - expert_ids.shape[1])))
    packed = jnp.concatenate([tokens, ids], axis=1)
    along = [packed] + [
        exchange(packed, expert_bits=0, shard_bits=d * inner) for d in range(1, outer)
    ]

    w_gate, w_up, w_down = (
        pltpu.with_memory_space_constraint(w[0], pltpu.HBM) for w in (w_gate, w_up, w_down)
    )
    shard_bytes = width * n_hidden * 2
    gate_held = pl.pallas_call(
        hold_kernel,
        name="hold_gate",
        out_shape=pltpu.VMEM((width, n_hidden), bf16),
        in_specs=[hbm],
        out_specs=vmem,
        scratch_shapes=[pltpu.SemaphoreType.DMA],
        compiler_params=pltpu.CompilerParams(vmem_limit_bytes=1 * MIB),
        cost_estimate=cost(4e9, shard_bytes),
    )(w_gate)

    buffers = pl.pallas_call(
        functools.partial(dispatch_kernel, outer, n_experts, width),
        name="dispatch",
        out_shape=[jax.ShapeDtypeStruct((per_expert, width), bf16)] * n_experts,
        in_specs=[vmem] * outer,
        out_specs=[vmem] * n_experts,
        compiler_params=pltpu.CompilerParams(vmem_limit_bytes=6 * MIB),
        cost_estimate=cost(4e8, 4 * MIB),
    )(*along)

    order = [(i, k) for i in range(inner) for k in range(n_experts)]
    row_parts = [
        buffers[k] if (i, k) == (0, 0) else exchange(buffers[k], expert_bits=k, shard_bits=i)
        for i, k in order
    ]

    high, low, up_held = pl.pallas_call(
        functools.partial(gates_kernel, outer, n_experts, width),
        name="gates_hold_up",
        out_shape=[
            jax.ShapeDtypeStruct((n_experts * per_expert, gathered), bf16),
            jax.ShapeDtypeStruct((n_experts * per_expert, gathered), bf16),
            pltpu.VMEM((width, n_hidden), bf16),
        ],
        in_specs=[vmem] * outer + [vmem, hbm],
        out_specs=[vmem] * 3,
        scratch_shapes=[pltpu.SemaphoreType.DMA],
        compiler_params=pltpu.CompilerParams(vmem_limit_bytes=6 * MIB),
        cost_estimate=cost(4e9, shard_bytes),
    )(*along, router.T, w_up)

    held = [pltpu.with_memory_space_constraint(w, pltpu.VMEM) for w in (gate_held, up_held)]
    out_tile = OUT_TILE
    out_parts = pl.pallas_call(
        functools.partial(ffn_kernel, parts),
        name="ffn",
        out_shape=[jax.ShapeDtypeStruct((per_expert, width), bf16)] * parts,
        in_specs=[vmem] * parts + [vmem, vmem, hbm],
        out_specs=[vmem] * parts,
        scratch_shapes=[
            pltpu.VMEM((width // out_tile, n_hidden, out_tile), bf16),
            pltpu.VMEM((n_rows, width), bf16),
            pltpu.VMEM((n_rows, n_hidden), bf16),
            pltpu.SemaphoreType.DMA((width // out_tile,)),
        ],
        compiler_params=pltpu.CompilerParams(vmem_limit_bytes=24 * MIB),
        cost_estimate=cost(6 * n_rows * width * n_hidden, 3 * shard_bytes),
    )(*row_parts, *held, w_down)

    back = [
        out_parts[j] if (i, k) == (0, 0) else exchange(out_parts[j], expert_bits=k, shard_bits=i)
        for j, (i, k) in enumerate(order)
    ]
    mixed = pl.pallas_call(
        functools.partial(combine_kernel, parts, n_experts, outer),
        name="combine",
        out_shape=[jax.ShapeDtypeStruct((local_tokens, width), bf16)] * outer,
        in_specs=[vmem] * (parts + 2),
        out_specs=[vmem] * outer,
        compiler_params=pltpu.CompilerParams(vmem_limit_bytes=20 * MIB),
        cost_estimate=cost(4 * n_rows * gathered * width, 4 * MIB),
    )(*back, high, low)
    home = [mixed[0]] + [
        exchange(mixed[d], expert_bits=0, shard_bits=d * inner) for d in range(1, outer)
    ]
    return pl.pallas_call(
        final_kernel,
        name="final",
        out_shape=jax.ShapeDtypeStruct((local_tokens, width), bf16),
        in_specs=[vmem] * outer,
        out_specs=vmem,
        compiler_params=pltpu.CompilerParams(vmem_limit_bytes=4 * MIB),
        cost_estimate=cost(1e6, MIB),
    )(*home)


def solution(mesh):
    placed = (
        P(("expert", "shard"), None),
        P(),
        P(("expert", "shard"), None),
        P("expert", None, "shard"),
        P("expert", None, "shard"),
        P("expert", "shard", None),
    )
    body = functools.partial(shards_program, mesh.shape["expert"], mesh.shape["shard"])
    return jax.shard_map(
        body, mesh=mesh, in_specs=placed, out_specs=P(("expert", "shard"), None), check_vma=False
    )
```

```python
import functools

import jax
import jax.numpy as jnp
from jax import lax
from jax.experimental import pallas as pl
from jax.experimental.pallas import tpu as pltpu
from jax.sharding import PartitionSpec as P


LANES = 128
HIDDEN_TILE = 256
OUT_TILE = 1024
LONG = 2e10
MIB = 1 << 20


def cost(flops, moved):
    return pl.CostEstimate(flops=int(flops), bytes_accessed=int(moved), transcendentals=0)


def dot(a, b, contract=(1, 0)):
    dims = (((contract[0],), (contract[1],)), ((), ()))
    return lax.dot_general(a, b, dims, preferred_element_type=jnp.float32)


def line_split(count):
    inner = 1
    while inner * inner * 4 <= count:
        inner *= 2
    return count // inner, inner


def swap(value, experts, shards, expert_bits, shard_bits):
    pairs = [
        (e * shards + s, (e ^ expert_bits) * shards + (s ^ shard_bits))
        for e in range(experts)
        for s in range(shards)
    ]
    return lax.ppermute(value, ("expert", "shard"), pairs)


def picks(ids_by_lane, first_expert, n_experts, blocks, slots_per):
    per_block = 2 * slots_per
    n_tokens = blocks * per_block
    rows = n_experts * blocks * slots_per
    row = lax.broadcasted_iota(jnp.int32, (rows, n_tokens), 0)
    token = lax.broadcasted_iota(jnp.int32, (rows, n_tokens), 1)
    expert = (first_expert ^ (row // (blocks * slots_per))).astype(jnp.float32)
    block = (row // slots_per) % blocks
    slot = (row % slots_per).astype(jnp.float32)
    is_first = ids_by_lane[0:1, :] == expert
    names = jnp.where(is_first | (ids_by_lane[1:2, :] == expert), 1.0, 0.0)
    earlier_token = lax.broadcasted_iota(jnp.int32, (n_tokens, n_tokens), 0)
    later_token = lax.broadcasted_iota(jnp.int32, (n_tokens, n_tokens), 1)
    earlier = jnp.where(
        (earlier_token < later_token)
        & (earlier_token // per_block == later_token // per_block),
        1.0,
        0.0,
    )
    before = dot(names.astype(jnp.bfloat16), earlier.astype(jnp.bfloat16))
    chosen = jnp.where((token // per_block == block) & (before == slot), names, 0.0)
    return chosen, is_first


def ids_to_lanes(packed_ids, blocks):
    n_tokens = packed_ids.shape[0]
    per_block = n_tokens // blocks
    lane = lax.broadcasted_iota(jnp.int32, (LANES, n_tokens), 0)
    token = lax.broadcasted_iota(jnp.int32, (LANES, n_tokens), 1)
    row = lax.broadcasted_iota(jnp.int32, (per_block, n_tokens), 1)
    lanes = jnp.zeros((per_block, n_tokens), jnp.float32)
    spread = jnp.where(lane == token % per_block, 1.0, 0.0).astype(jnp.bfloat16)
    spreads = dot(packed_ids, spread)
    for block in range(blocks):
        mine = spreads[block * per_block : (block + 1) * per_block]
        lanes = lanes + jnp.where(row // per_block == block, mine, 0.0)
    return lanes


def gather_blocks(refs):
    return jnp.concatenate([ref[...].astype(jnp.float32) for ref in refs], axis=0).astype(
        jnp.bfloat16
    )


def dispatch_kernel(blocks, n_experts, width, *refs):
    packed = gather_blocks(refs[:blocks])
    out_refs = refs[blocks:]
    slots_per = packed.shape[0] // blocks // 2
    per_expert = blocks * slots_per
    lanes = ids_to_lanes(packed[:, width:], blocks)
    chosen, _ = picks(lanes, lax.axis_index("expert"), n_experts, blocks, slots_per)
    rows = dot(chosen.astype(jnp.bfloat16), packed[:, :width]).astype(jnp.bfloat16)
    for k in range(n_experts):
        out_refs[k][...] = rows[k * per_expert : (k + 1) * per_expert]


def pack_kernel(tokens_ref, ids_ref, packed_ref):
    n_tokens, width = tokens_ref.shape
    packed_ref[:, :width] = tokens_ref[...]
    lane = lax.broadcasted_iota(jnp.int32, (LANES, n_tokens), 0)
    token = lax.broadcasted_iota(jnp.int32, (LANES, n_tokens), 1)
    spread = jnp.where(lane == token, 1.0, 0.0).astype(jnp.bfloat16)
    ids = ids_ref[...].astype(jnp.float32).astype(jnp.bfloat16)
    rows = jnp.concatenate([ids, jnp.zeros((n_tokens - 2, n_tokens), jnp.bfloat16)], axis=0)
    packed_ref[:, width:] = dot(rows, spread, (1, 1)).astype(jnp.bfloat16)


def gates_kernel(blocks, n_experts, width, *refs):
    router_ref, high_ref, low_ref = refs[blocks:]
    packed = gather_blocks(refs[:blocks])
    slots_per = packed.shape[0] // blocks // 2
    lanes = ids_to_lanes(packed[:, width:], blocks)
    chosen, is_first = picks(lanes, lax.axis_index("expert"), n_experts, blocks, slots_per)
    logits = dot(router_ref[...], packed[:, :width], (1, 1))
    expert = lax.broadcasted_iota(jnp.int32, logits.shape, 0).astype(jnp.float32)
    first = jnp.sum(jnp.where(lanes[0:1, :] == expert, logits, 0.0), axis=0, keepdims=True)
    second = jnp.sum(jnp.where(lanes[1:2, :] == expert, logits, 0.0), axis=0, keepdims=True)
    gate = 1.0 / (1.0 + jnp.exp(-(first - second)))
    weights = chosen * jnp.where(is_first, gate, 1.0 - gate)
    high = weights.astype(jnp.bfloat16)
    high_ref[...] = high
    low_ref[...] = (weights - high.astype(jnp.float32)).astype(jnp.bfloat16)


def ffn_kernel(parts, tile_width, out_tile, *refs):
    row_refs = refs[:parts]
    gate_ref, up_ref, down_ref = refs[parts : parts + 3]
    out_refs = refs[parts + 3 : 2 * parts + 3]
    rows, hidden = refs[2 * parts + 3 :]
    per_part = row_refs[0].shape[0]
    for part in range(parts):
        rows[pl.ds(part * per_part, per_part), :] = row_refs[part][...]

    @pl.loop(0, hidden.shape[1] // tile_width)
    def _(tile):
        columns = pl.ds(pl.multiple_of(tile * tile_width, tile_width), tile_width)
        gate = dot(rows[...], gate_ref[:, columns])
        up = dot(rows[...], up_ref[:, columns])
        hidden[:, columns] = (gate / (1.0 + jnp.exp(-gate)) * up).astype(jnp.bfloat16)

    @pl.loop(0, down_ref.shape[1] // out_tile)
    def _(tile):
        columns = pl.ds(pl.multiple_of(tile * out_tile, out_tile), out_tile)
        result = dot(hidden[...], down_ref[:, columns]).astype(jnp.bfloat16)
        for part in range(parts):
            out_refs[part][:, columns] = result[part * per_part : (part + 1) * per_part]


def combine_kernel(parts, n_experts, blocks, *refs):
    part_refs = refs[:parts]
    high_ref, low_ref = refs[parts : parts + 2]
    out_refs = refs[parts + 2 :]
    inner = parts // n_experts
    rows = jnp.concatenate([ref[...] for ref in part_refs], axis=0)
    high = jnp.concatenate([high_ref[...]] * inner, axis=0)
    low = jnp.concatenate([low_ref[...]] * inner, axis=0)
    mixed = dot(high, rows, (0, 0)) + dot(low, rows, (0, 0))
    per_block = mixed.shape[0] // blocks
    for block in range(blocks):
        out_refs[block][...] = mixed[block * per_block : (block + 1) * per_block].astype(
            jnp.bfloat16
        )


def final_kernel(*refs):
    total = refs[0][...].astype(jnp.float32)
    for ref in refs[1:-1]:
        total = total + ref[...].astype(jnp.float32)
    refs[-1][...] = total.astype(jnp.bfloat16)


def shards_program(n_expert_axis, n_shard_axis, tokens, router, expert_ids, w_gate, w_up, w_down):
    local_tokens, width = tokens.shape
    n_experts = router.shape[1]
    outer, inner = line_split(n_shard_axis)
    slots_per = local_tokens // 2
    per_expert = outer * slots_per
    parts = inner * n_experts
    n_rows = parts * per_expert
    gathered = outer * local_tokens
    n_hidden = w_gate.shape[2]
    bf16 = jnp.bfloat16
    vmem = pl.BlockSpec(memory_space=pltpu.VMEM)
    hbm = pl.BlockSpec(memory_space=pltpu.HBM)

    def exchange(value, expert_bits, shard_bits):
        return swap(value, n_expert_axis, n_shard_axis, expert_bits, shard_bits)

    w_gate, w_up, w_down = w_gate[0], w_up[0], w_down[0]
    packed = pl.pallas_call(
        pack_kernel,
        name="pack",
        out_shape=jax.ShapeDtypeStruct((local_tokens, width + LANES), bf16),
        in_specs=[vmem] * 2,
        out_specs=vmem,
        compiler_params=pltpu.CompilerParams(vmem_limit_bytes=2 * MIB),
        cost_estimate=cost(LONG, MIB),
    )(*(pltpu.with_memory_space_constraint(v, pltpu.HBM) for v in (tokens, expert_ids.T)))
    along = [packed] + [exchange(packed, 0, d * inner) for d in range(1, outer)]

    tile_width = HIDDEN_TILE if n_hidden % HIDDEN_TILE == 0 else LANES
    buffers = pl.pallas_call(
        functools.partial(dispatch_kernel, outer, n_experts, width),
        name="dispatch",
        out_shape=[jax.ShapeDtypeStruct((per_expert, width), bf16)] * n_experts,
        in_specs=[vmem] * outer,
        out_specs=[vmem] * n_experts,
        compiler_params=pltpu.CompilerParams(vmem_limit_bytes=6 * MIB),
        cost_estimate=cost(LONG, 4 * MIB),
    )(*along)

    order = [(i, k) for i in range(inner) for k in range(n_experts)]
    row_parts = [buffers[k] if (i, k) == (0, 0) else exchange(buffers[k], k, i) for i, k in order]

    high, low = pl.pallas_call(
        functools.partial(gates_kernel, outer, n_experts, width),
        name="gates",
        out_shape=[jax.ShapeDtypeStruct((n_experts * per_expert, gathered), bf16)] * 2,
        in_specs=[vmem] * (outer + 1),
        out_specs=[vmem] * 2,
        compiler_params=pltpu.CompilerParams(vmem_limit_bytes=6 * MIB),
        cost_estimate=cost(LONG, MIB),
    )(*along, router.T)

    out_parts = pl.pallas_call(
        functools.partial(ffn_kernel, parts, tile_width, OUT_TILE),
        name="ffn",
        out_shape=[jax.ShapeDtypeStruct((per_expert, width), bf16)] * parts,
        in_specs=[vmem] * (parts + 3),
        out_specs=[vmem] * parts,
        scratch_shapes=[pltpu.VMEM((n_rows, width), bf16), pltpu.VMEM((n_rows, n_hidden), bf16)],
        compiler_params=pltpu.CompilerParams(vmem_limit_bytes=5 * MIB),
        cost_estimate=cost(6 * n_rows * width * n_hidden, 6 * width * n_hidden),
    )(*row_parts, w_gate, w_up, w_down)

    back = [
        out_parts[j] if (i, k) == (0, 0) else exchange(out_parts[j], k, i)
        for j, (i, k) in enumerate(order)
    ]
    mixed = pl.pallas_call(
        functools.partial(combine_kernel, parts, n_experts, outer),
        name="combine",
        out_shape=[jax.ShapeDtypeStruct((local_tokens, width), bf16)] * outer,
        in_specs=[vmem] * (parts + 2),
        out_specs=[vmem] * outer,
        compiler_params=pltpu.CompilerParams(vmem_limit_bytes=20 * MIB),
        cost_estimate=cost(4 * n_rows * gathered * width, 4 * MIB),
    )(*back, high, low)
    home = [mixed[0]] + [exchange(mixed[d], 0, d * inner) for d in range(1, outer)]
    return pl.pallas_call(
        final_kernel,
        name="final",
        out_shape=jax.ShapeDtypeStruct((local_tokens, width), bf16),
        in_specs=[vmem] * outer,
        out_specs=vmem,
        compiler_params=pltpu.CompilerParams(vmem_limit_bytes=4 * MIB),
        cost_estimate=cost(1e6, MIB),
    )(*home)


def solution(mesh):
    placed = (
        P(("expert", "shard"), None),
        P(),
        P(("expert", "shard"), None),
        P("expert", None, "shard"),
        P("expert", None, "shard"),
        P("expert", "shard", None),
    )
    experts, shards = mesh.shape["expert"], mesh.shape["shard"]

    def body(*args):
        return shards_program(experts, shards, *args)

    return jax.shard_map(
        body, mesh=mesh, in_specs=placed, out_specs=P(("expert", "shard"), None), check_vma=False
    )
```

```python
import functools

import jax
import jax.numpy as jnp
from jax import lax
from jax.experimental import pallas as pl
from jax.experimental.pallas import tpu as pltpu
from jax.sharding import PartitionSpec as P


LANES = 128
HIDDEN_TILE = 256
OUT_TILE = 1024
LONG = 6e10
MIB = 1 << 20


def cost(flops, moved):
    return pl.CostEstimate(flops=int(flops), bytes_accessed=int(moved), transcendentals=0)


def dot(a, b, contract=(1, 0)):
    dims = (((contract[0],), (contract[1],)), ((), ()))
    return lax.dot_general(a, b, dims, preferred_element_type=jnp.float32)


def line_split(count):
    inner = 1
    while inner * inner * 4 <= count:
        inner *= 2
    return count // inner, inner


def swap(value, experts, shards, expert_bits, shard_bits):
    pairs = [
        (e * shards + s, (e ^ expert_bits) * shards + (s ^ shard_bits))
        for e in range(experts)
        for s in range(shards)
    ]
    return lax.ppermute(value, ("expert", "shard"), pairs)


def picks(ids_by_lane, first_expert, n_experts, blocks, slots_per):
    per_block = 2 * slots_per
    n_tokens = blocks * per_block
    rows = n_experts * blocks * slots_per
    row = lax.broadcasted_iota(jnp.int32, (rows, n_tokens), 0)
    token = lax.broadcasted_iota(jnp.int32, (rows, n_tokens), 1)
    expert = (first_expert ^ (row // (blocks * slots_per))).astype(jnp.float32)
    block = (row // slots_per) % blocks
    slot = (row % slots_per).astype(jnp.float32)
    is_first = ids_by_lane[0:1, :] == expert
    names = jnp.where(is_first | (ids_by_lane[1:2, :] == expert), 1.0, 0.0)
    earlier_token = lax.broadcasted_iota(jnp.int32, (n_tokens, n_tokens), 0)
    later_token = lax.broadcasted_iota(jnp.int32, (n_tokens, n_tokens), 1)
    earlier = jnp.where(
        (earlier_token < later_token)
        & (earlier_token // per_block == later_token // per_block),
        1.0,
        0.0,
    )
    before = dot(names.astype(jnp.bfloat16), earlier.astype(jnp.bfloat16))
    chosen = jnp.where((token // per_block == block) & (before == slot), names, 0.0)
    return chosen, is_first


def ids_to_lanes(packed_ids, blocks):
    n_tokens = packed_ids.shape[0]
    per_block = n_tokens // blocks
    lane = lax.broadcasted_iota(jnp.int32, (LANES, n_tokens), 0)
    token = lax.broadcasted_iota(jnp.int32, (LANES, n_tokens), 1)
    row = lax.broadcasted_iota(jnp.int32, (per_block, n_tokens), 1)
    lanes = jnp.zeros((per_block, n_tokens), jnp.float32)
    spread = jnp.where(lane == token % per_block, 1.0, 0.0).astype(jnp.bfloat16)
    spreads = dot(packed_ids, spread)
    for block in range(blocks):
        mine = spreads[block * per_block : (block + 1) * per_block]
        lanes = lanes + jnp.where(row // per_block == block, mine, 0.0)
    return lanes


def gather_blocks(refs):
    return jnp.concatenate([ref[...].astype(jnp.float32) for ref in refs], axis=0).astype(
        jnp.bfloat16
    )


def dispatch_kernel(blocks, n_experts, width, *refs):
    packed = gather_blocks(refs[:blocks])
    out_refs = refs[blocks:]
    slots_per = packed.shape[0] // blocks // 2
    per_expert = blocks * slots_per
    lanes = ids_to_lanes(packed[:, width:], blocks)
    chosen, _ = picks(lanes, lax.axis_index("expert"), n_experts, blocks, slots_per)
    rows = dot(chosen.astype(jnp.bfloat16), packed[:, :width]).astype(jnp.bfloat16)
    for k in range(n_experts):
        out_refs[k][...] = rows[k * per_expert : (k + 1) * per_expert]


def pack_kernel(tokens_ref, ids_ref, packed_ref):
    n_tokens, width = tokens_ref.shape
    packed_ref[:, :width] = tokens_ref[...]
    lane = lax.broadcasted_iota(jnp.int32, (LANES, n_tokens), 0)
    token = lax.broadcasted_iota(jnp.int32, (LANES, n_tokens), 1)
    spread = jnp.where(lane == token, 1.0, 0.0).astype(jnp.bfloat16)
    ids = ids_ref[...].astype(jnp.float32).astype(jnp.bfloat16)
    rows = jnp.concatenate([ids, jnp.zeros((n_tokens - 2, n_tokens), jnp.bfloat16)], axis=0)
    packed_ref[:, width:] = dot(rows, spread, (1, 1)).astype(jnp.bfloat16)


def gates_kernel(blocks, n_experts, width, *refs):
    router_ref, high_ref, low_ref = refs[blocks:]
    packed = gather_blocks(refs[:blocks])
    slots_per = packed.shape[0] // blocks // 2
    lanes = ids_to_lanes(packed[:, width:], blocks)
    chosen, is_first = picks(lanes, lax.axis_index("expert"), n_experts, blocks, slots_per)
    logits = dot(router_ref[...], packed[:, :width], (1, 1))
    expert = lax.broadcasted_iota(jnp.int32, logits.shape, 0).astype(jnp.float32)
    first = jnp.sum(jnp.where(lanes[0:1, :] == expert, logits, 0.0), axis=0, keepdims=True)
    second = jnp.sum(jnp.where(lanes[1:2, :] == expert, logits, 0.0), axis=0, keepdims=True)
    gate = 1.0 / (1.0 + jnp.exp(-(first - second)))
    weights = chosen * jnp.where(is_first, gate, 1.0 - gate)
    high = weights.astype(jnp.bfloat16)
    high_ref[...] = high
    low_ref[...] = (weights - high.astype(jnp.float32)).astype(jnp.bfloat16)


def ffn_kernel(parts, halves, tile_width, out_tile, *refs):
    pieces = parts * halves
    row_refs = refs[:pieces]
    gate_ref, up_ref, down_ref = refs[pieces : pieces + 3]
    out_refs = refs[pieces + 3 : 2 * pieces + 3]
    rows, hidden = refs[2 * pieces + 3 :]
    per_piece = row_refs[0].shape[0]
    per_part = per_piece * halves
    for part in range(parts):
        mine = row_refs[part * halves : (part + 1) * halves]
        rows[pl.ds(part * per_part, per_part), :] = gather_blocks(mine)

    @pl.loop(0, hidden.shape[1] // tile_width)
    def _(tile):
        columns = pl.ds(pl.multiple_of(tile * tile_width, tile_width), tile_width)
        gate = dot(rows[...], gate_ref[:, columns])
        up = dot(rows[...], up_ref[:, columns])
        hidden[:, columns] = (gate / (1.0 + jnp.exp(-gate)) * up).astype(jnp.bfloat16)

    @pl.loop(0, down_ref.shape[1] // out_tile)
    def _(tile):
        columns = pl.ds(pl.multiple_of(tile * out_tile, out_tile), out_tile)
        result = dot(hidden[...], down_ref[:, columns])
        for piece in range(pieces):
            mine = result[piece * per_piece : (piece + 1) * per_piece]
            out_refs[piece][:, columns] = mine.astype(jnp.bfloat16)


def combine_kernel(parts, n_experts, blocks, *refs):
    high_ref, low_ref = refs[parts : parts + 2]
    out_refs = refs[parts + 2 :]
    inner = parts // n_experts
    rows = gather_blocks(refs[:parts])
    high = jnp.concatenate([high_ref[...]] * inner, axis=0)
    low = jnp.concatenate([low_ref[...]] * inner, axis=0)
    mixed = dot(high, rows, (0, 0)) + dot(low, rows, (0, 0))
    per_block = mixed.shape[0] // blocks
    for block in range(blocks):
        out_refs[block][...] = mixed[block * per_block : (block + 1) * per_block].astype(
            jnp.bfloat16
        )


def final_kernel(*refs):
    total = refs[0][...].astype(jnp.float32)
    for ref in refs[1:-1]:
        total = total + ref[...].astype(jnp.float32)
    refs[-1][...] = total.astype(jnp.bfloat16)


def shards_program(n_expert_axis, n_shard_axis, tokens, router, expert_ids, w_gate, w_up, w_down):
    local_tokens, width = tokens.shape
    n_experts = router.shape[1]
    outer, inner = line_split(n_shard_axis)
    slots_per = local_tokens // 2
    per_expert = outer * slots_per
    parts = inner * n_experts
    n_rows = parts * per_expert
    n_hidden = w_gate.shape[2]
    bf16 = jnp.bfloat16
    vmem = pl.BlockSpec(memory_space=pltpu.VMEM)
    hbm = pl.BlockSpec(memory_space=pltpu.HBM)

    def exchange(value, expert_bits, shard_bits):
        return swap(value, n_expert_axis, n_shard_axis, expert_bits, shard_bits)

    w_gate, w_up, w_down = w_gate[0], w_up[0], w_down[0]
    packed = pl.pallas_call(
        pack_kernel,
        name="pack",
        out_shape=jax.ShapeDtypeStruct((local_tokens, width + LANES), bf16),
        in_specs=[vmem] * 2,
        out_specs=vmem,
        compiler_params=pltpu.CompilerParams(vmem_limit_bytes=2 * MIB),
        cost_estimate=cost(LONG, MIB),
    )(*(pltpu.with_memory_space_constraint(v, pltpu.HBM) for v in (tokens, expert_ids.T)))
    along = [packed] + [exchange(packed, 0, d * inner) for d in range(1, outer)]

    tile_width = HIDDEN_TILE if n_hidden % HIDDEN_TILE == 0 else LANES
    halves = 2
    per_half = outer // halves
    piece_rows = per_half * slots_per
    order = [(i, k) for i in range(inner) for k in range(n_experts)]

    def dispatch(half):
        return pl.pallas_call(
            functools.partial(dispatch_kernel, per_half, n_experts, width),
            out_shape=[jax.ShapeDtypeStruct((piece_rows, width), bf16)] * n_experts,
            in_specs=[vmem] * per_half,
            out_specs=[vmem] * n_experts,
            compiler_params=pltpu.CompilerParams(vmem_limit_bytes=6 * MIB),
            cost_estimate=cost(4e8, 4 * MIB),
        )(*along[half * per_half : (half + 1) * per_half])

    def weights(half):
        n_tokens = per_half * local_tokens
        return pl.pallas_call(
            functools.partial(gates_kernel, per_half, n_experts, width),
            out_shape=[jax.ShapeDtypeStruct((n_experts * piece_rows, n_tokens), bf16)] * 2,
            in_specs=[vmem] * (per_half + 1),
            out_specs=[vmem] * 2,
            compiler_params=pltpu.CompilerParams(vmem_limit_bytes=6 * MIB),
            cost_estimate=cost(4e8, MIB),
        )(*along[half * per_half : (half + 1) * per_half], router.T)

    arrived = []
    for half in range(halves):
        buffers = dispatch(half)
        arrived.append(
            [buffers[k] if (i, k) == (0, 0) else exchange(buffers[k], k, i) for i, k in order]
        )
    combine_weights = [weights(half) for half in range(halves)]

    pieces = parts * halves
    sent = pl.pallas_call(
        functools.partial(ffn_kernel, parts, halves, tile_width, OUT_TILE),
        name="ffn",
        out_shape=[jax.ShapeDtypeStruct((piece_rows, width), bf16)] * pieces,
        in_specs=[vmem] * (pieces + 3),
        out_specs=[vmem] * pieces,
        scratch_shapes=[pltpu.VMEM((n_rows, width), bf16), pltpu.VMEM((n_rows, n_hidden), bf16)],
        compiler_params=pltpu.CompilerParams(vmem_limit_bytes=5 * MIB),
        cost_estimate=cost(6 * n_rows * width * n_hidden, 6 * width * n_hidden),
    )(*(arrived[half][j] for j in range(parts) for half in range(halves)), w_gate, w_up, w_down)

    mixed = []
    for half in range(halves):
        mine = sent[half::halves]
        back = [
            mine[j] if (i, k) == (0, 0) else exchange(mine[j], k, i)
            for j, (i, k) in enumerate(order)
        ]
        mixed += pl.pallas_call(
            functools.partial(combine_kernel, parts, n_experts, per_half),
            out_shape=[jax.ShapeDtypeStruct((local_tokens, width), bf16)] * per_half,
            in_specs=[vmem] * (parts + 2),
            out_specs=[vmem] * per_half,
            compiler_params=pltpu.CompilerParams(vmem_limit_bytes=20 * MIB),
            cost_estimate=cost(4e8, 4 * MIB),
        )(*back, *combine_weights[half])
    home = [mixed[0]] + [exchange(mixed[d], 0, d * inner) for d in range(1, outer)]
    return pl.pallas_call(
        final_kernel,
        name="final",
        out_shape=jax.ShapeDtypeStruct((local_tokens, width), bf16),
        in_specs=[vmem] * outer,
        out_specs=vmem,
        compiler_params=pltpu.CompilerParams(vmem_limit_bytes=4 * MIB),
        cost_estimate=cost(1e6, MIB),
    )(*home)


def solution(mesh):
    placed = (
        P(("expert", "shard"), None),
        P(),
        P(("expert", "shard"), None),
        P("expert", None, "shard"),
        P("expert", None, "shard"),
        P("expert", "shard", None),
    )
    experts, shards = mesh.shape["expert"], mesh.shape["shard"]

    def body(*args):
        return shards_program(experts, shards, *args)

    return jax.shard_map(
        body, mesh=mesh, in_specs=placed, out_specs=P(("expert", "shard"), None), check_vma=False
    )
```

```python
import functools

import jax
import jax.numpy as jnp
from jax import lax
from jax.experimental import pallas as pl
from jax.experimental.pallas import tpu as pltpu
from jax.sharding import PartitionSpec as P


LANES = 128
HIDDEN_TILE = 256
OUT_TILE = 1024
LONG = 6e10
MIB = 1 << 20


def cost(flops, moved):
    return pl.CostEstimate(flops=int(flops), bytes_accessed=int(moved), transcendentals=0)


def dot(a, b, contract=(1, 0)):
    dims = (((contract[0],), (contract[1],)), ((), ()))
    return lax.dot_general(a, b, dims, preferred_element_type=jnp.float32)


def line_split(count):
    inner = 1
    while inner * inner * 4 <= count:
        inner *= 2
    return count // inner, inner


def swap(value, experts, shards, expert_bits, shard_bits):
    pairs = [
        (e * shards + s, (e ^ expert_bits) * shards + (s ^ shard_bits))
        for e in range(experts)
        for s in range(shards)
    ]
    return lax.ppermute(value, ("expert", "shard"), pairs)


def picks(ids_by_lane, first_expert, n_experts, blocks, slots_per):
    per_block = 2 * slots_per
    n_tokens = blocks * per_block
    rows = n_experts * blocks * slots_per
    row = lax.broadcasted_iota(jnp.int32, (rows, n_tokens), 0)
    token = lax.broadcasted_iota(jnp.int32, (rows, n_tokens), 1)
    expert = (first_expert ^ (row // (blocks * slots_per))).astype(jnp.float32)
    block = (row // slots_per) % blocks
    slot = (row % slots_per).astype(jnp.float32)
    is_first = ids_by_lane[0:1, :] == expert
    names = jnp.where(is_first | (ids_by_lane[1:2, :] == expert), 1.0, 0.0)
    earlier_token = lax.broadcasted_iota(jnp.int32, (n_tokens, n_tokens), 0)
    later_token = lax.broadcasted_iota(jnp.int32, (n_tokens, n_tokens), 1)
    earlier = jnp.where(
        (earlier_token < later_token)
        & (earlier_token // per_block == later_token // per_block),
        1.0,
        0.0,
    )
    before = dot(names.astype(jnp.bfloat16), earlier.astype(jnp.bfloat16))
    chosen = jnp.where((token // per_block == block) & (before == slot), names, 0.0)
    return chosen, is_first


def ids_to_lanes(packed_ids, blocks):
    n_tokens = packed_ids.shape[0]
    per_block = n_tokens // blocks
    lane = lax.broadcasted_iota(jnp.int32, (LANES, n_tokens), 0)
    token = lax.broadcasted_iota(jnp.int32, (LANES, n_tokens), 1)
    row = lax.broadcasted_iota(jnp.int32, (per_block, n_tokens), 1)
    lanes = jnp.zeros((per_block, n_tokens), jnp.float32)
    spread = jnp.where(lane == token % per_block, 1.0, 0.0).astype(jnp.bfloat16)
    spreads = dot(packed_ids, spread)
    for block in range(blocks):
        mine = spreads[block * per_block : (block + 1) * per_block]
        lanes = lanes + jnp.where(row // per_block == block, mine, 0.0)
    return lanes


def gather_blocks(refs):
    return jnp.concatenate([ref[...].astype(jnp.float32) for ref in refs], axis=0).astype(
        jnp.bfloat16
    )


def dispatch_kernel(blocks, n_experts, width, wanted, *refs):
    packed = gather_blocks(refs[:blocks])
    out_refs = refs[blocks:]
    slots_per = packed.shape[0] // blocks // 2
    per_expert = blocks * slots_per
    lanes = ids_to_lanes(packed[:, width:], blocks)
    chosen, _ = picks(lanes, lax.axis_index("expert"), n_experts, blocks, slots_per)
    rows = dot(chosen.astype(jnp.bfloat16), packed[:, :width])
    for out_ref, (k, first, count) in zip(out_refs, wanted):
        start = k * per_expert + first
        out_ref[...] = rows[start : start + count].astype(jnp.bfloat16)


def pack_kernel(tokens_ref, ids_ref, packed_ref):
    n_tokens, width = tokens_ref.shape
    packed_ref[:, :width] = tokens_ref[...]
    lane = lax.broadcasted_iota(jnp.int32, (LANES, n_tokens), 0)
    token = lax.broadcasted_iota(jnp.int32, (LANES, n_tokens), 1)
    spread = jnp.where(lane == token, 1.0, 0.0).astype(jnp.bfloat16)
    ids = ids_ref[...].astype(jnp.float32).astype(jnp.bfloat16)
    rows = jnp.concatenate([ids, jnp.zeros((n_tokens - 2, n_tokens), jnp.bfloat16)], axis=0)
    packed_ref[:, width:] = dot(rows, spread, (1, 1)).astype(jnp.bfloat16)


def gates_kernel(blocks, n_experts, width, *refs):
    router_ref, high_ref, low_ref = refs[blocks:]
    packed = gather_blocks(refs[:blocks])
    slots_per = packed.shape[0] // blocks // 2
    lanes = ids_to_lanes(packed[:, width:], blocks)
    chosen, is_first = picks(lanes, lax.axis_index("expert"), n_experts, blocks, slots_per)
    logits = dot(router_ref[...], packed[:, :width], (1, 1))
    expert = lax.broadcasted_iota(jnp.int32, logits.shape, 0).astype(jnp.float32)
    first = jnp.sum(jnp.where(lanes[0:1, :] == expert, logits, 0.0), axis=0, keepdims=True)
    second = jnp.sum(jnp.where(lanes[1:2, :] == expert, logits, 0.0), axis=0, keepdims=True)
    gate = 1.0 / (1.0 + jnp.exp(-(first - second)))
    weights = chosen * jnp.where(is_first, gate, 1.0 - gate)
    high = weights.astype(jnp.bfloat16)
    high_ref[...] = high
    low_ref[...] = (weights - high.astype(jnp.float32)).astype(jnp.bfloat16)


def ffn_kernel(piece_counts, tile_width, out_tile, *refs):
    pieces = sum(piece_counts)
    row_refs = refs[:pieces]
    gate_ref, up_ref, down_ref = refs[pieces : pieces + 3]
    out_refs = refs[pieces + 3 : 2 * pieces + 3]
    rows, hidden = refs[2 * pieces + 3 :]
    per_part = rows.shape[0] // len(piece_counts)
    taken = 0
    for part, count in enumerate(piece_counts):
        mine = row_refs[taken : taken + count]
        rows[pl.ds(part * per_part, per_part), :] = gather_blocks(mine)
        taken += count

    @pl.loop(0, hidden.shape[1] // tile_width)
    def _(tile):
        columns = pl.ds(pl.multiple_of(tile * tile_width, tile_width), tile_width)
        gate = dot(rows[...], gate_ref[:, columns])
        up = dot(rows[...], up_ref[:, columns])
        hidden[:, columns] = (gate / (1.0 + jnp.exp(-gate)) * up).astype(jnp.bfloat16)

    @pl.loop(0, down_ref.shape[1] // out_tile)
    def _(tile):
        columns = pl.ds(pl.multiple_of(tile * out_tile, out_tile), out_tile)
        result = dot(hidden[...], down_ref[:, columns])
        first = 0
        for out_ref in out_refs:
            count = out_ref.shape[0]
            out_ref[:, columns] = result[first : first + count].astype(jnp.bfloat16)
            first += count


def combine_kernel(parts, n_experts, blocks, half, *refs):
    high_ref, low_ref = refs[parts : parts + 2]
    out_refs = refs[parts + 2 :]
    inner = parts // n_experts
    count = high_ref.shape[0] // n_experts
    rows = []
    for ref in refs[:parts]:
        first = half * count if ref.shape[0] > count else 0
        rows.append(ref[...].astype(jnp.float32)[first : first + count])
    rows = jnp.concatenate(rows, axis=0).astype(jnp.bfloat16)
    high = jnp.concatenate([high_ref[...]] * inner, axis=0)
    low = jnp.concatenate([low_ref[...]] * inner, axis=0)
    mixed = dot(high, rows, (0, 0)) + dot(low, rows, (0, 0))
    per_block = mixed.shape[0] // blocks
    for block in range(blocks):
        out_refs[block][...] = mixed[block * per_block : (block + 1) * per_block].astype(
            jnp.bfloat16
        )


def final_kernel(*refs):
    total = refs[0][...].astype(jnp.float32)
    for ref in refs[1:-1]:
        total = total + ref[...].astype(jnp.float32)
    refs[-1][...] = total.astype(jnp.bfloat16)


def shards_program(n_expert_axis, n_shard_axis, tokens, router, expert_ids, w_gate, w_up, w_down):
    local_tokens, width = tokens.shape
    n_experts = router.shape[1]
    outer, inner = line_split(n_shard_axis)
    slots_per = local_tokens // 2
    per_expert = outer * slots_per
    parts = inner * n_experts
    n_rows = parts * per_expert
    n_hidden = w_gate.shape[2]
    bf16 = jnp.bfloat16
    vmem = pl.BlockSpec(memory_space=pltpu.VMEM)
    hbm = pl.BlockSpec(memory_space=pltpu.HBM)

    def exchange(value, expert_bits, shard_bits):
        return swap(value, n_expert_axis, n_shard_axis, expert_bits, shard_bits)

    w_gate, w_up, w_down = w_gate[0], w_up[0], w_down[0]
    packed = pl.pallas_call(
        pack_kernel,
        name="pack",
        out_shape=jax.ShapeDtypeStruct((local_tokens, width + LANES), bf16),
        in_specs=[vmem] * 2,
        out_specs=vmem,
        compiler_params=pltpu.CompilerParams(vmem_limit_bytes=2 * MIB),
        cost_estimate=cost(LONG, MIB),
    )(*(pltpu.with_memory_space_constraint(v, pltpu.HBM) for v in (tokens, expert_ids.T)))
    along = [packed] + [exchange(packed, 0, d * inner) for d in range(1, outer)]

    tile_width = HIDDEN_TILE if n_hidden % HIDDEN_TILE == 0 else LANES
    halves = 2
    per_half = outer // halves
    piece_rows = per_half * slots_per
    order = [(i, k) for i in range(inner) for k in range(n_experts)]

    split, whole = plane_groups(inner, n_experts)

    def dispatch(blocks, wanted):
        outs = pl.pallas_call(
            functools.partial(dispatch_kernel, blocks, n_experts, width, tuple(wanted)),
            out_shape=[jax.ShapeDtypeStruct((w[2], width), bf16) for w in wanted],
            in_specs=[vmem] * blocks,
            out_specs=[vmem] * len(wanted),
            compiler_params=pltpu.CompilerParams(vmem_limit_bytes=8 * MIB),
            cost_estimate=cost(4e8, 4 * MIB),
        )(*along[:blocks])
        return dict(zip(wanted, outs))

    def weights(half):
        n_tokens = per_half * local_tokens
        return pl.pallas_call(
            functools.partial(gates_kernel, per_half, n_experts, width),
            out_shape=[jax.ShapeDtypeStruct((n_experts * piece_rows, n_tokens), bf16)] * 2,
            in_specs=[vmem] * (per_half + 1),
            out_specs=[vmem] * 2,
            compiler_params=pltpu.CompilerParams(vmem_limit_bytes=6 * MIB),
            cost_estimate=cost(4e8, MIB),
        )(*along[half * per_half : (half + 1) * per_half], router.T)

    split_experts = sorted({k for _, k in split})
    whole_experts = sorted({k for _, k in whole} | {0})
    near_rows = dispatch(per_half, [(k, 0, piece_rows) for k in split_experts])
    late_rows = dispatch(
        outer,
        [(k, piece_rows, piece_rows) for k in split_experts]
        + [(k, 0, per_expert) for k in whole_experts],
    )
    row_pieces = []
    for i, k in order:
        if (i, k) in split:
            row_pieces.append(exchange(near_rows[k, 0, piece_rows], k, i))
            row_pieces.append(exchange(late_rows[k, piece_rows, piece_rows], k, i))
        elif (i, k) == (0, 0):
            row_pieces.append(late_rows[k, 0, per_expert])
        else:
            row_pieces.append(exchange(late_rows[k, 0, per_expert], k, i))
    piece_counts = tuple(2 if p in split else 1 for p in order)
    combine_weights = [weights(half) for half in range(halves)]

    sent = pl.pallas_call(
        functools.partial(ffn_kernel, piece_counts, tile_width, OUT_TILE),
        name="ffn",
        out_shape=[jax.ShapeDtypeStruct(piece.shape, bf16) for piece in row_pieces],
        in_specs=[vmem] * (len(row_pieces) + 3),
        out_specs=[vmem] * len(row_pieces),
        scratch_shapes=[pltpu.VMEM((n_rows, width), bf16), pltpu.VMEM((n_rows, n_hidden), bf16)],
        compiler_params=pltpu.CompilerParams(vmem_limit_bytes=5 * MIB),
        cost_estimate=cost(6 * n_rows * width * n_hidden, 6 * width * n_hidden),
    )(*row_pieces, w_gate, w_up, w_down)

    back = ([], [])
    left = list(sent)
    for i, k in order:
        if (i, k) in split:
            back[0].append(exchange(left.pop(0), k, i))
            back[1].append(exchange(left.pop(0), k, i))
        else:
            mine = left.pop(0)
            if (i, k) != (0, 0):
                mine = exchange(mine, k, i)
            back[0].append(mine)
            back[1].append(mine)
    mixed = []
    for half in range(halves):
        mixed += pl.pallas_call(
            functools.partial(combine_kernel, parts, n_experts, per_half, half),
            out_shape=[jax.ShapeDtypeStruct((local_tokens, width), bf16)] * per_half,
            in_specs=[vmem] * (parts + 2),
            out_specs=[vmem] * per_half,
            compiler_params=pltpu.CompilerParams(vmem_limit_bytes=20 * MIB),
            cost_estimate=cost(4e8, 4 * MIB),
        )(*back[half], *combine_weights[half])
    home = [mixed[0]] + [exchange(mixed[d], 0, d * inner) for d in range(1, outer)]
    return pl.pallas_call(
        final_kernel,
        name="final",
        out_shape=jax.ShapeDtypeStruct((local_tokens, width), bf16),
        in_specs=[vmem] * outer,
        out_specs=vmem,
        compiler_params=pltpu.CompilerParams(vmem_limit_bytes=4 * MIB),
        cost_estimate=cost(1e6, MIB),
    )(*home)


def plane_groups(inner, n_experts):
    others = [(i, k) for i in range(inner) for k in range(n_experts) if (i, k) != (0, 0)]
    far = [p for p in others if p[0] and p[1] > 1]
    near = [p for p in others if not p[0] and p[1] < 2]
    by_k = [p for p in others if not p[0] and p[1] > 1]
    by_i = [p for p in others if p[0] and p[1] < 2]
    pairs = [p for pair in zip(by_k, by_i) for p in pair]
    pairs += by_k[len(by_i) :] + by_i[len(by_k) :]
    count = len(pairs) // 2
    return far + pairs[:count], pairs[count:] + near


def solution(mesh):
    placed = (
        P(("expert", "shard"), None),
        P(),
        P(("expert", "shard"), None),
        P("expert", None, "shard"),
        P("expert", None, "shard"),
        P("expert", "shard", None),
    )
    experts, shards = mesh.shape["expert"], mesh.shape["shard"]

    def body(*args):
        return shards_program(experts, shards, *args)

    return jax.shard_map(
        body, mesh=mesh, in_specs=placed, out_specs=P(("expert", "shard"), None), check_vma=False
    )
```
